32 devices in a mesh: dp: 2 (over x), ep: 16 (over y, z, core).
Axes of the slice: x: 2, y: 2, z: 4, core: 2. Of those that a mesh axis runs over, the one named last changes fastest.
Arguments:
- x: bfloat16 [2, 16, 256, 3584], P('dp', 'ep'), parts along dimension 0
- expert: int32 [2, 16, 256, 8], P('dp', 'ep'), parts along dimension 0
- slot: int32 [2, 16, 256, 8], P('dp', 'ep'), parts along dimension 0
- gate: float32 [2, 16, 256, 8], P('dp', 'ep'), parts along dimension 0
- w_gate: bfloat16 [48, 3584, 2048], P('ep')
- w_up: bfloat16 [48, 3584, 2048], P('ep')
- w_down: bfloat16 [48, 2048, 3584], P('ep')
- s_gate: bfloat16 [3584, 2048], replicated
- s_up: bfloat16 [3584, 2048], replicated
- s_down: bfloat16 [2048, 3584], replicated
Outputs:
- y: bfloat16 [2, 16, 256, 3584], P('dp', 'ep'), parts along dimension 0
There are 2 independent parts. The reference program is written for one: setup_inputs(seed, part) draws one part's arguments, and reference() takes and returns one part's arrays. A program takes and returns all parts, laid end to end along the dimension named above; an argument that names none is the same for every part.
All inputs are finite; a program needn't handle non-finite values.
Results may differ from the reference program's by a relative error of at most 0.009.
Values are sent between devices in bfloat16 or wider.
A program may use at most 2 GiB of HBM per device.

```python
import jax
import jax.numpy as jnp

MEMBERS = 16
TOKENS = 256
D = 3584
FF = 2048
TOP = 8
EXPERTS = 48
SHARED_FF = 2048
SLOTS = 5 * TOKENS * TOP // (4 * EXPERTS)


def setup_inputs(seed: int = 0, part: int = 0) -> dict:
    own, k1, k2, k3, k4, k5, k6 = jax.random.split(jax.random.key(seed), 7)
    kx, ke, kl, kg = jax.random.split(jax.random.fold_in(own, part), 4)
    devices = (1, MEMBERS)
    place = jax.random.permutation(kl, jnp.arange(EXPERTS, dtype=jnp.uint32))
    slow = ((EXPERTS + (9 * place) % EXPERTS) << ((9 * place) // EXPERTS)) // EXPERTS
    wait = (jax.random.bits(ke, (*devices, TOKENS, EXPERTS), jnp.uint32) >> 10) * slow
    expert = jnp.argsort(wait, axis=-1)[..., :TOP].astype(jnp.int32)
    chosen = jax.nn.one_hot(expert, EXPERTS, dtype=jnp.int32)
    in_line = jnp.cumsum(chosen.reshape(*devices, TOKENS * TOP, EXPERTS), axis=2) - 1
    slot = jnp.sum(in_line.reshape(chosen.shape) * chosen, axis=-1)

    def one(key, rows, columns):
        return (jax.random.normal(key, (rows, columns), jnp.float32) * rows**-0.5).astype(jnp.bfloat16)

    def weights(key, rows, columns):
        return jax.lax.map(lambda k: one(k, rows, columns), jax.random.split(key, EXPERTS))

    return {
        "x": jax.random.normal(kx, (*devices, TOKENS, D), jnp.float32).astype(jnp.bfloat16),
        "expert": expert,
        "slot": slot,
        "gate": jax.nn.softmax(jax.random.normal(kg, expert.shape, jnp.float32)),
        "w_gate": weights(k1, D, FF),
        "w_up": weights(k2, D, FF),
        "w_down": weights(k3, FF, D),
        "s_gate": one(k4, D, SHARED_FF),
        "s_up": one(k5, D, SHARED_FF),
        "s_down": one(k6, SHARED_FF, D),
    }


def einsum(form, a, b):
    return jnp.einsum(form, a.astype(jnp.float32), b.astype(jnp.float32))


def for_all(x, s_gate, s_up, s_down):
    h = jax.nn.silu(einsum("...d,df->...f", x, s_gate)) * einsum("...d,df->...f", x, s_up)
    return einsum("...f,fd->...d", h.astype(jnp.bfloat16), s_down)


def reference(x, expert, slot, gate, w_gate, w_up, w_down, s_gate, s_up, s_down):
    to_expert = jax.nn.one_hot(expert, EXPERTS, dtype=jnp.bfloat16)
    to_slot = jax.nn.one_hot(slot, SLOTS, dtype=jnp.bfloat16)
    weighted = to_expert * gate[..., None].astype(jnp.bfloat16)
    dispatch = einsum("abtke,abtkc->abtec", to_expert, to_slot).astype(jnp.bfloat16)
    combine = einsum("abtke,abtkc->abtec", weighted, to_slot).astype(jnp.bfloat16)
    z = einsum("abtec,abtd->aebcd", dispatch, x).astype(jnp.bfloat16)
    h = jax.nn.silu(einsum("aebcd,edf->aebcf", z, w_gate))
    h = (h * einsum("aebcd,edf->aebcf", z, w_up)).astype(jnp.bfloat16)
    out = einsum("aebcf,efd->aebcd", h, w_down).astype(jnp.bfloat16)
    y = einsum("abtec,aebcd->abtd", combine, out)
    return (y + for_all(x, s_gate, s_up, s_down)).astype(jnp.bfloat16)
```

```python
import jax
import jax.numpy as jnp
from jax import lax
from jax.sharding import PartitionSpec as P


def mm(form, a, b):
    return jnp.einsum(form, a, b, preferred_element_type=jnp.float32)


def solution(mesh):
    def step(x, expert, slot, gate, w_gate, w_up, w_down, s_gate, s_up, s_down):
        members = mesh.shape["ep"]
        experts, (tokens, top) = w_gate.shape[0], expert.shape[2:]
        slots = 5 * tokens * top // (4 * experts)
        own = experts // members
        pad = -(-slots // 8) * 8

        def device(x, expert, slot, gate, w_gate, w_up, w_down, s_gate, s_up, s_down):
            x, expert, slot, gate = x[0, 0], expert[0, 0], slot[0, 0], gate[0, 0]
            me = lax.axis_index("ep")
            code = jnp.where(slot < slots, expert * pad + slot, -1).astype(jnp.float32)
            info = jnp.concatenate([code, gate.astype(jnp.bfloat16).astype(jnp.float32)], axis=1)
            info = lax.all_gather(info, "ep")
            xs = lax.all_gather(x, "ep")
            row = info[..., :top].astype(jnp.int32) - me * own * pad
            weight = info[..., top:]
            rows = own * pad
            take = jnp.zeros((members, rows, tokens), jnp.float32)
            give = jnp.zeros((members, tokens, rows), jnp.float32)
            for j in range(top):
                r = row[..., j]
                take += (r[:, None, :] == jnp.arange(rows)[None, :, None]).astype(jnp.float32)
                give += jnp.where(r[..., None] == jnp.arange(rows), weight[..., j, None], 0.0)
            take, give = take.astype(jnp.bfloat16), give.astype(jnp.bfloat16)
            z = mm("srt,std->srd", take, xs).astype(jnp.bfloat16)
            z = z.reshape(members, own, pad, -1).transpose(1, 0, 2, 3).reshape(own, members * pad, -1)
            h = jax.nn.silu(mm("erd,edf->erf", z, w_gate)) * mm("erd,edf->erf", z, w_up)
            out = mm("erf,efd->erd", h.astype(jnp.bfloat16), w_down).astype(jnp.bfloat16)
            out = out.reshape(own, members, pad, -1).transpose(1, 0, 2, 3).reshape(members, rows, -1)
            part = mm("str,srd->std", give, out).astype(jnp.bfloat16)
            y = lax.psum_scatter(part, "ep", scatter_dimension=0)
            hs = jax.nn.silu(mm("td,df->tf", x, s_gate)) * mm("td,df->tf", x, s_up)
            shared = mm("tf,fd->td", hs.astype(jnp.bfloat16), s_down)
            return (y.astype(jnp.float32) + shared).astype(jnp.bfloat16)[None, None]

        tok, exp, rep = P("dp", "ep"), P("ep"), P()
        return jax.shard_map(
            device, mesh=mesh,
            in_specs=(tok, tok, tok, tok, exp, exp, exp, rep, rep, rep),
            out_specs=tok, check_vma=False,
        )(x, expert, slot, gate, w_gate, w_up, w_down, s_gate, s_up, s_down)

    return step
```

```python
import functools

import jax
import jax.numpy as jnp
from jax import lax
from jax.experimental import pallas as pl
from jax.experimental.pallas import tpu as pltpu
from jax.sharding import PartitionSpec as P

MESH = pl.DeviceIdType.MESH
F32, BF16 = jnp.float32, jnp.bfloat16
CHIPS = 8
HALF = 256
UNIT = 2 * HALF
TILE = 256


def dot(a, b):
    return jnp.dot(a, b, preferred_element_type=F32)


def chip_at(pos):
    return pos + pos // 4 * (11 - 2 * pos)


def places():
    me = lax.axis_index("ep")
    core, pos = me % 2, chip_at(me // 2)

    def device(pos, core):
        return (lax.axis_index("dp"), 2 * chip_at(pos) + core)

    right, left = device((pos + 1) % CHIPS, core), device((pos + CHIPS - 1) % CHIPS, core)
    return core, pos, right, left, device(pos, 1 - core)


def meet(devices):
    barrier = pltpu.get_barrier_semaphore()
    for d in devices:
        pl.semaphore_signal(barrier, inc=1, device_id=d, device_id_type=MESH)
    pl.semaphore_wait(barrier, len(devices))


def gather_up(
    x_ref, take_ref, wg_ref, wu_ref, sg_ref, su_ref, all_ref, h_ref, hs_ref,
    acc, acc_s, xbuf, z, wbuf, hbuf,
    send_sem, recv_sem, psend_sem, precv_sem, load_sem, w_sem, h_sem,
):
    own, total, ff = acc.shape[1:]
    tokens, d = x_ref.shape
    units = d // UNIT
    sources = 2 * CHIPS
    pad = total // sources
    core, pos, right, left, partner = places()
    ahead = (right, left)
    meet((right, left, partner))

    def origin(way, hop):
        return (pos - hop + CHIPS) % CHIPS if way == 0 else (pos + hop) % CHIPS

    def cols(j, way):
        return pl.ds(pl.multiple_of(j * UNIT + way * HALF, HALF), HALF)

    def ring(j, way, hop):
        here = all_ref.at[core, origin(way, hop), :, cols(j, way)]
        src = x_ref.at[:, cols(j, way)] if hop == 0 else here
        return pltpu.make_async_remote_copy(
            src_ref=src, dst_ref=here, send_sem=send_sem.at[way, j, hop],
            recv_sem=recv_sem.at[way, j, hop], device_id=ahead[way], device_id_type=MESH)

    def arrival(j, way, hop):
        there = all_ref.at[core, origin(way, hop), :, cols(j, way)]
        return pltpu.make_async_remote_copy(
            src_ref=there, dst_ref=there, send_sem=send_sem.at[way, j, hop - 1],
            recv_sem=recv_sem.at[way, j, hop - 1], device_id=ahead[way], device_id_type=MESH)

    def pair(j, way, hop):
        here = all_ref.at[core, origin(way, hop), :, cols(j, way)]
        src = x_ref.at[:, cols(j, way)] if hop == 0 else here
        return pltpu.make_async_remote_copy(
            src_ref=src, dst_ref=here, send_sem=psend_sem.at[way, j, hop],
            recv_sem=precv_sem.at[way, j, hop], device_id=partner, device_id_type=MESH)

    def pair_arrival(j, way, hop):
        there = all_ref.at[1 - core, origin(way, hop), :, cols(j, way)]
        return pltpu.make_async_remote_copy(
            src_ref=there, dst_ref=there, send_sem=psend_sem.at[way, j, hop],
            recv_sem=precv_sem.at[way, j, hop], device_id=partner, device_id_type=MESH)

    def load(j, color, place):
        wide = pl.ds(pl.multiple_of(j * UNIT, UNIT), UNIT)
        s = color * CHIPS + place
        return pltpu.make_async_copy(all_ref.at[color, place, :, wide], xbuf.at[s], load_sem.at[s])

    def load_own(j):
        wide = pl.ds(pl.multiple_of(j * UNIT, UNIT), UNIT)
        s = core * CHIPS + pos
        return pltpu.make_async_copy(x_ref.at[:, wide], xbuf.at[s], load_sem.at[s])

    mats = [sg_ref, su_ref] + [m.at[e] for e in range(own) for m in (wg_ref, wu_ref)]
    count = len(mats)

    def weight(j, k):
        rows = pl.ds(pl.multiple_of(j * UNIT, UNIT), UNIT)
        return pltpu.make_async_copy(mats[k].at[rows, :], wbuf.at[k % 2], w_sem.at[k % 2])

    def send(j, hop):
        for way in range(2):
            if hop > 0:
                arrival(j, way, hop).wait_recv()
            if hop < CHIPS - 1:
                ring(j, way, hop).start()
            pair(j, way, hop).start()

    def product(j, k):
        weight(j, k).wait()
        if k + 1 < count:
            weight(j, k + 1).start()
        else:
            @pl.when(j + 1 < units)
            def _():
                weight(j + 1, 0).start()
        w = wbuf.at[k % 2]
        e, up = (k - 2) // 2, k % 2
        if k < 2:
            lhs, total_ref = xbuf.at[core * CHIPS + pos], acc_s.at[up]
        else:
            lhs, total_ref = z.at[e], acc.at[up, e]

        @pl.loop(0, ff // TILE)
        def _(n):
            at = pl.ds(pl.multiple_of(n * TILE, TILE), TILE)
            total_ref[:, at] += dot(lhs[...], w[:, at])

    def finish(e):
        gate = acc_s.at[0] if e == own else acc.at[0, e]
        up = acc_s.at[1] if e == own else acc.at[1, e]
        n_rows = tokens if e == own else total
        out = hs_ref if e == own else h_ref.at[e]

        def put(n, b):
            at = pl.ds(pl.multiple_of(n * TILE, TILE), TILE)
            return pltpu.make_async_copy(hbuf.at[b, pl.ds(0, n_rows)], out.at[:, at], h_sem.at[b])

        @pl.loop(0, ff // TILE, step=2)
        def _(n):
            for b in range(2):
                at = pl.ds(pl.multiple_of((n + b) * TILE, TILE), TILE)

                @pl.when(n > 0)
                def _():
                    put(n + b - 2, b).wait()
                g = gate[:, at]
                hbuf[b, pl.ds(0, n_rows)] = (g * jax.nn.sigmoid(g) * up[:, at]).astype(BF16)
                put(n + b, b).start()
        for b in range(2):
            put(ff // TILE - 2 + b, b).wait()

    weight(0, 0).start()

    @pl.loop(0, ff // TILE)
    def _(n):
        at = pl.ds(pl.multiple_of(n * TILE, TILE), TILE)
        for g in range(2):
            acc_s[g, :, at] = jnp.zeros((tokens, TILE), F32)
            for e in range(own):
                acc[g, e, :, at] = jnp.zeros((total, TILE), F32)

    @pl.loop(0, units + 3)
    def _(u):
        for i in range(7):
            back, hop = (0, i // 2) if i % 2 == 0 else (1, i // 2 + 4)

            @pl.when(jnp.logical_and(u - back >= 0, u - back < units))
            def _():
                send(u - back, hop)
            now = u - 2
            if i == 0:
                @pl.when(jnp.logical_and(now >= 0, now < units))
                def _():
                    send(now, CHIPS - 1)
                    load_own(now).start()
                    for hop in range(1, CHIPS):
                        load(now, core, origin(0, hop)).start()
                    for hop in range(CHIPS - 1):
                        for way in range(2):
                            pair_arrival(now, way, hop).wait_recv()
                    for hop in (0, 2, 3, 4, 5, 6):
                        load(now, 1 - core, origin(0, hop)).start()

                @pl.when(jnp.logical_and(now - 1 >= 0, now - 1 < units))
                def _():
                    product(now - 1, count - 1)
            else:
                @pl.when(jnp.logical_and(now >= 0, now < units))
                def _():
                    if i == 1:
                        for way in range(2):
                            pair_arrival(now, way, CHIPS - 1).wait_recv()
                        for hop in (1, CHIPS - 1):
                            load(now, 1 - core, origin(0, hop)).start()
                        load_own(now).wait()
                        for hop in range(1, CHIPS):
                            load(now, core, origin(0, hop)).wait()
                        for hop in range(CHIPS):
                            load(now, 1 - core, origin(0, hop)).wait()
                        for s in range(sources):
                            rows = dot(take_ref[s], xbuf[s]).astype(BF16)
                            for e in range(own):
                                z[e, pl.ds(s * pad, pad), :] = rows[e * pad:(e + 1) * pad]
                        product(now, 0)
                        product(now, 1)
                    else:
                        product(now, i)

    for e in (own, *range(own)):
        finish(e)

    @pl.loop(0, units)
    def _(j):
        for way in range(2):
            for hop in range(CHIPS - 1):
                ring(j, way, hop).wait_send()
            for hop in range(CHIPS):
                pair(j, way, hop).wait_send()


def down_scatter(
    h_ref, hs_ref, give_ref, wd_ref, sd_ref, y_ref,
    part, shared, psend, precv, outs, wbuf, rbuf,
    send_sem, recv_sem, psend_sem, precv_sem, w_sem,
):
    own, total, ff = h_ref.shape
    tokens, d = y_ref.shape
    units = d // UNIT
    sources = 2 * CHIPS
    pad = total // sources
    core, pos, right, left, partner = places()
    ahead = (right, left)
    meet((right, left, partner))

    mats = [sd_ref] + [wd_ref.at[e] for e in range(own)]
    count = len(mats)

    def weight(j, k):
        wide = pl.ds(pl.multiple_of(j * UNIT, UNIT), UNIT)
        return pltpu.make_async_copy(mats[k].at[:, wide], wbuf.at[k % 2], w_sem.at[k % 2])

    def bound(way, hop):
        return (pos - 1 - hop + 2 * CHIPS) % CHIPS if way == 0 else (pos + 1 + hop) % CHIPS

    def ring(j, way, hop):
        return pltpu.make_async_remote_copy(
            src_ref=rbuf.at[way, j, hop], dst_ref=rbuf.at[way, j, hop + 1],
            send_sem=send_sem.at[way, j, hop], recv_sem=recv_sem.at[way, j, hop],
            device_id=ahead[way], device_id_type=MESH)

    def arrival(j, way, hop):
        return pltpu.make_async_remote_copy(
            src_ref=rbuf.at[way, j, hop - 1], dst_ref=rbuf.at[way, j, hop],
            send_sem=send_sem.at[way, j, hop - 1], recv_sem=recv_sem.at[way, j, hop - 1],
            device_id=ahead[way], device_id_type=MESH)

    def pair(j):
        b = j % 2
        return pltpu.make_async_remote_copy(
            src_ref=psend.at[b], dst_ref=precv.at[b], send_sem=psend_sem.at[b],
            recv_sem=precv_sem.at[b], device_id=partner, device_id_type=MESH)

    def send(j, hop):
        for way in range(2):
            half = pl.ds(way * HALF, HALF)
            mine = part[j % 3, bound(way, hop), :, half]
            if hop > 0:
                arrival(j, way, hop).wait_recv()
                mine += rbuf[way, j, hop].astype(F32)
            if hop < CHIPS - 1:
                rbuf[way, j, hop] = mine.astype(BF16)
                ring(j, way, hop).start()
            else:
                at = pl.ds(pl.multiple_of(j * UNIT + way * HALF, HALF), HALF)
                y_ref[:, at] = mine.astype(BF16)

    def product(j, k):
        weight(j, k).wait()
        if k + 1 < count:
            weight(j, k + 1).start()
        else:
            @pl.when(j + 1 < units)
            def _():
                weight(j + 1, 0).start()
        for n in range(UNIT // TILE):
            at = pl.ds(n * TILE, TILE)
            if k == 0:
                shared[:, at] = dot(hs_ref[...], wbuf[k % 2, :, at])
            else:
                e = k - 1
                r = dot(h_ref[e], wbuf[k % 2, :, at]).astype(BF16)
                for s in range(sources):
                    outs[s, pl.ds(e * pad, pad), at] = r[s * pad:(s + 1) * pad]

    def combine(j):
        for place in range(CHIPS):
            s = core * CHIPS + place
            part[j % 3, place] = dot(give_ref[s], outs[s])
            o = (1 - core) * CHIPS + place
            psend[j % 2, place] = dot(give_ref[o], outs[o]).astype(BF16)
        pair(j).start()
        part[j % 3, pos] += shared[...]

    weight(0, 0).start()

    @pl.loop(0, units + 3)
    def _(u):
        for i in range(7):
            if i == 0:
                @pl.when(jnp.logical_and(u - 3 >= 0, u - 3 < units))
                def _():
                    send(u - 3, CHIPS - 1)

                @pl.when(jnp.logical_and(u - 1 >= 0, u - 1 < units))
                def _():
                    pair(u - 1).wait()
                    for place in range(CHIPS):
                        part[(u - 1) % 3, place] += precv[(u - 1) % 2, place].astype(F32)
            back, hop = (1, i // 2) if i % 2 == 0 else (2, i // 2 + 4)

            @pl.when(jnp.logical_and(u - back >= 0, u - back < units))
            def _():
                send(u - back, hop)

            @pl.when(u < units)
            def _():
                if 1 <= i <= count:
                    product(u, i - 1)
                if i == 6:
                    combine(u)

    @pl.loop(0, units)
    def _(j):
        for way in range(2):
            for hop in range(CHIPS - 1):
                ring(j, way, hop).wait_send()


def solution(mesh):
    def step(x, expert, slot, gate, w_gate, w_up, w_down, s_gate, s_up, s_down):
        members = mesh.shape["ep"]
        experts, (tokens, top) = w_gate.shape[0], expert.shape[2:]
        d, ff = w_gate.shape[1:]
        slots = 5 * tokens * top // (4 * experts)
        own = experts // members
        pad = -(-slots // 8) * 8
        rows, total, units = own * pad, members * pad, d // UNIT
        order = [2 * chip_at(pos) + core for core in range(2) for pos in range(CHIPS)]
        dma, anywhere, vmem = pltpu.SemaphoreType.DMA, pl.BlockSpec(memory_space=pl.ANY), pl.BlockSpec(memory_space=pltpu.VMEM)

        def device(x, expert, slot, gate, w_gate, w_up, w_down, s_gate, s_up, s_down):
            x, expert, slot, gate = x[0, 0], expert[0, 0], slot[0, 0], gate[0, 0]
            me = lax.axis_index("ep")
            code = jnp.where(slot < slots, expert * pad + slot, -1).astype(F32)
            info = jnp.concatenate([code, gate.astype(BF16).astype(F32)], axis=1)
            info = lax.all_gather(info, "ep")
            info = jnp.stack([info[m] for m in order])
            row = info[..., :top].astype(jnp.int32) - me * own * pad
            weight = info[..., top:]
            take = jnp.zeros((members, rows, tokens), F32)
            give = jnp.zeros((members, tokens, rows), F32)
            for j in range(top):
                r = row[..., j]
                take += (r[:, None, :] == jnp.arange(rows)[None, :, None]).astype(F32)
                give += jnp.where(r[..., None] == jnp.arange(rows), weight[..., j, None], 0.0)
            take, give = take.astype(BF16), give.astype(BF16)
            _, h, hs = pl.pallas_call(
                gather_up,
                name="gather_up",
                out_shape=(
                    jax.ShapeDtypeStruct((2, CHIPS, tokens, d), BF16),
                    jax.ShapeDtypeStruct((own, total, ff), BF16),
                    jax.ShapeDtypeStruct((tokens, ff), BF16),
                ),
                in_specs=[anywhere, vmem] + [anywhere] * 4,
                out_specs=(anywhere,) * 3,
                scratch_shapes=[
                    pltpu.VMEM((2, own, total, ff), F32),
                    pltpu.VMEM((2, tokens, ff), F32),
                    pltpu.VMEM((members, tokens, UNIT), BF16),
                    pltpu.VMEM((own, total, UNIT), BF16),
                    pltpu.VMEM((2, UNIT, ff), BF16),
                    pltpu.VMEM((2, total, TILE), BF16),
                    dma((2, units, CHIPS)), dma((2, units, CHIPS)), dma((2, units, CHIPS)),
                    dma((2, units, CHIPS)), dma((members,)), dma((2,)), dma((2,)),
                ],
                compiler_params=pltpu.CompilerParams(
                    collective_id=0, has_side_effects=True, vmem_limit_bytes=67_043_328),
            )(x, take, w_gate, w_up, s_gate, s_up)
            y = pl.pallas_call(
                down_scatter,
                name="down_scatter",
                out_shape=jax.ShapeDtypeStruct((tokens, d), BF16),
                in_specs=[vmem] * 3 + [anywhere] * 2,
                out_specs=vmem,
                scratch_shapes=[
                    pltpu.VMEM((3, CHIPS, tokens, UNIT), F32),
                    pltpu.VMEM((tokens, UNIT), F32),
                    pltpu.VMEM((2, CHIPS, tokens, UNIT), BF16),
                    pltpu.VMEM((2, CHIPS, tokens, UNIT), BF16),
                    pltpu.VMEM((members, rows, UNIT), BF16),
                    pltpu.VMEM((2, ff, UNIT), BF16),
                    pltpu.VMEM((2, units, CHIPS, tokens, HALF), BF16),
                    dma((2, units, CHIPS)), dma((2, units, CHIPS)), dma((2,)), dma((2,)), dma((2,)),
                ],
                compiler_params=pltpu.CompilerParams(
                    collective_id=1, has_side_effects=True, vmem_limit_bytes=67_043_328),
            )(h, hs, give, w_down, s_down)
            return y[None, None]

        tok, exp, rep = P("dp", "ep"), P("ep"), P()
        return jax.shard_map(
            device, mesh=mesh,
            in_specs=(tok, tok, tok, tok, exp, exp, exp, rep, rep, rep),
            out_specs=tok, check_vma=False,
        )(x, expert, slot, gate, w_gate, w_up, w_down, s_gate, s_up, s_down)

    return step
```

```python
import functools

import jax
import jax.numpy as jnp
from jax import lax
from jax.experimental import pallas as pl
from jax.experimental.pallas import tpu as pltpu
from jax.sharding import PartitionSpec as P

MESH = pl.DeviceIdType.MESH
F32, BF16 = jnp.float32, jnp.bfloat16
CHIPS = 8
HALF = 256
UNIT = 2 * HALF
TILE = 256
STRIP = 256
DEPTH = 5


def dot(a, b):
    return jnp.dot(a, b, preferred_element_type=F32)


def tdot(a, b):
    return lax.dot_general(a, b, (((0,), (0,)), ((), ())), preferred_element_type=F32)


def chip_at(pos):
    return pos + pos // 4 * (11 - 2 * pos)


def places():
    me = lax.axis_index("ep")
    core, pos = me % 2, chip_at(me // 2)

    def device(pos, core):
        return (lax.axis_index("dp"), 2 * chip_at(pos) + core)

    right, left = device((pos + 1) % CHIPS, core), device((pos + CHIPS - 1) % CHIPS, core)
    return core, pos, right, left, device(pos, 1 - core)


def meet(devices):
    barrier = pltpu.get_barrier_semaphore()
    for d in devices:
        pl.semaphore_signal(barrier, inc=1, device_id=d, device_id_type=MESH)
    pl.semaphore_wait(barrier, len(devices))


def gather_up(
    x_ref, info_ref, wg_ref, wu_ref, sg_ref, su_ref, all_ref, h_ref, hs_ref, give_ref,
    acc, acc_s, xbuf, z, wbuf, hbuf, info, take, give,
    send_sem, recv_sem, psend_sem, precv_sem, info_sem, load_sem, w_sem, h_sem, give_sem,
):
    own, total, ff = acc.shape[1:]
    tokens, d = x_ref.shape
    top = info_ref.shape[0] // 2
    units = d // UNIT
    sources = 2 * CHIPS
    pad = total // sources
    core, pos, right, left, partner = places()
    ahead = (right, left)
    meet((right, left, partner))

    def origin(way, hop):
        return (pos - hop + CHIPS) % CHIPS if way == 0 else (pos + hop) % CHIPS

    def block(j, way, hop, color):
        at = pl.ds(pl.multiple_of(j * UNIT + way * HALF, HALF), HALF)
        return all_ref.at[color, origin(way, hop), :, at]

    def mine(j, way):
        return x_ref.at[:, pl.ds(pl.multiple_of(j * UNIT + way * HALF, HALF), HALF)]

    def ring(j, way, hop, src=None):
        here = block(j, way, hop, core)
        return pltpu.make_async_remote_copy(
            src_ref=here if src is None else src, dst_ref=here, send_sem=send_sem.at[way, j, hop],
            recv_sem=recv_sem.at[way, j, hop], device_id=ahead[way], device_id_type=MESH)

    def arrival(j, way, hop):
        there = block(j, way, hop, core)
        return pltpu.make_async_remote_copy(
            src_ref=there, dst_ref=there, send_sem=send_sem.at[way, j, hop - 1],
            recv_sem=recv_sem.at[way, j, hop - 1], device_id=ahead[way], device_id_type=MESH)

    def pair(j, way, hop, src=None):
        here = block(j, way, hop, core)
        return pltpu.make_async_remote_copy(
            src_ref=here if src is None else src, dst_ref=here, send_sem=psend_sem.at[way, j, hop],
            recv_sem=precv_sem.at[way, j, hop], device_id=partner, device_id_type=MESH)

    def pair_arrival(j, way, hop):
        there = block(j, way, hop, 1 - core)
        return pltpu.make_async_remote_copy(
            src_ref=there, dst_ref=there, send_sem=psend_sem.at[way, j, hop],
            recv_sem=precv_sem.at[way, j, hop], device_id=partner, device_id_type=MESH)

    def note(hop, to_pair, src=None):
        here = info.at[core, origin(0, hop)]
        return pltpu.make_async_remote_copy(
            src_ref=here if src is None else src, dst_ref=here, send_sem=info_sem.at[to_pair, 0, hop],
            recv_sem=info_sem.at[to_pair, 1, hop], device_id=partner if to_pair else right, device_id_type=MESH)

    def note_arrival(hop, to_pair):
        there = info.at[1 - core if to_pair else core, origin(0, hop)]
        n = hop if to_pair else hop - 1
        return pltpu.make_async_remote_copy(
            src_ref=there, dst_ref=there, send_sem=info_sem.at[to_pair, 0, n],
            recv_sem=info_sem.at[to_pair, 1, n], device_id=partner if to_pair else right, device_id_type=MESH)

    def load(j, color, place):
        wide = pl.ds(pl.multiple_of(j * UNIT, UNIT), UNIT)
        s = color * CHIPS + place
        return pltpu.make_async_copy(all_ref.at[color, place, :, wide], xbuf.at[s], load_sem.at[s])

    def load_own(j):
        wide = pl.ds(pl.multiple_of(j * UNIT, UNIT), UNIT)
        s = core * CHIPS + pos
        return pltpu.make_async_copy(x_ref.at[:, wide], xbuf.at[s], load_sem.at[s])

    last = 2 * own + 1

    def weight(j, k, mat):
        rows = pl.ds(pl.multiple_of(j * UNIT, UNIT), UNIT)
        return pltpu.make_async_copy(mat.at[rows, :], wbuf.at[k % 2], w_sem.at[k % 2])

    def send(j, hop):
        @pl.when(hop == 0)
        def _():
            @pl.when(j == 0)
            def _():
                note(0, 0, info_ref).start()
                note(0, 1, info_ref).start()
            for way in range(2):
                ring(j, way, 0, mine(j, way)).start()
                pair(j, way, 0, mine(j, way)).start()

        @pl.when(hop > 0)
        def _():
            @pl.when(j == 0)
            def _():
                note_arrival(hop, 0).wait_recv()
                note(hop, 0).start()
                note(hop, 1).start()
            for way in range(2):
                arrival(j, way, hop).wait_recv()
                ring(j, way, hop).start()
                pair(j, way, hop).start()

    def accumulate(lhs, w, total_ref):
        for n in range(0, ff, UNIT):
            at = pl.ds(n, UNIT)
            total_ref[:, at] += dot(lhs[...], w[:, at])

    def product(j, k):
        weight(j, k, wg_ref.at[0]).wait()
        e = (k - 1) // 2

        @pl.when(jnp.logical_and(k < last, k % 2 == 1))
        def _():
            weight(j, k + 1, wg_ref.at[e]).start()

        @pl.when(jnp.logical_and(k < last, k % 2 == 0))
        def _():
            weight(j, k + 1, wu_ref.at[e]).start()

        @pl.when(jnp.logical_and(k == last, j + 1 < units))
        def _():
            weight(j + 1, 0, sg_ref).start()
        accumulate(z.at[(k - 2) // 2], wbuf.at[k % 2], acc.at[k % 2, (k - 2) // 2])

    def shared(j):
        weight(j, 0, sg_ref).wait()
        weight(j, 1, su_ref).start()
        accumulate(xbuf.at[core * CHIPS + pos], wbuf.at[0], acc_s.at[0])
        weight(j, 1, su_ref).wait()
        weight(j, 2, wg_ref.at[0]).start()
        accumulate(xbuf.at[core * CHIPS + pos], wbuf.at[1], acc_s.at[1])

    def route():
        note_arrival(CHIPS - 1, 0).wait_recv()
        note(CHIPS - 1, 1).start()
        for hop in range(CHIPS):
            note_arrival(hop, 1).wait_recv()
        info[core, pos] = info_ref[...]
        base = (lax.axis_index("ep") * own * pad).astype(F32)

        @pl.loop(0, sources)
        def _(s):
            here = info[s // CHIPS, s % CHIPS]
            row = lax.broadcasted_iota(jnp.int32, (own * pad, tokens), 0).astype(F32)
            picked = jnp.zeros((own * pad, tokens), F32)
            gates = jnp.zeros((own * pad, tokens), F32)
            for n in range(top):
                hit = row == here[n:n + 1] - base
                picked = jnp.where(hit, 1.0, picked)
                gates = jnp.where(hit, here[top + n:top + n + 1], gates)
            take[s] = picked.astype(BF16)
            give[s] = gates.astype(BF16)
        pltpu.make_async_copy(give, give_ref, give_sem.at[0]).start()

    def dispatch(j):
        for way in range(2):
            pair_arrival(j, way, CHIPS - 1).wait_recv()
        for hop in (1, CHIPS - 1):
            load(j, 1 - core, origin(0, hop)).start()
        load_own(j).wait()
        for hop in range(1, CHIPS):
            load(j, core, origin(0, hop)).wait()
        for hop in range(CHIPS):
            load(j, 1 - core, origin(0, hop)).wait()
        for s in range(sources):
            rows = dot(take[s], xbuf[s]).astype(BF16)
            for e in range(own):
                z[e, pl.ds(s * pad, pad), :] = rows[e * pad:(e + 1) * pad]

    def fetch(j):
        for way in range(2):
            arrival(j, way, CHIPS - 1).wait_recv()
            pair(j, way, CHIPS - 1).start()
        load_own(j).start()
        for hop in range(1, CHIPS):
            load(j, core, origin(0, hop)).start()
        for hop in range(CHIPS - 1):
            for way in range(2):
                pair_arrival(j, way, hop).wait_recv()
        for hop in (0, *range(2, CHIPS - 1)):
            load(j, 1 - core, origin(0, hop)).start()

    def finish(e):
        gate = acc_s.at[0] if e == own else acc.at[0, e]
        up = acc_s.at[1] if e == own else acc.at[1, e]
        n_rows = tokens if e == own else total
        out = hs_ref if e == own else h_ref.at[e]

        def put(n, b):
            at = pl.ds(pl.multiple_of(n * TILE, TILE), TILE)
            return pltpu.make_async_copy(hbuf.at[b, pl.ds(0, n_rows)], out.at[:, at], h_sem.at[b])

        @pl.loop(0, ff // TILE, step=2)
        def _(n):
            for b in range(2):
                at = pl.ds(pl.multiple_of((n + b) * TILE, TILE), TILE)

                @pl.when(n > 0)
                def _():
                    put(n + b - 2, b).wait()
                g = 0.5 * gate[:, at]
                hbuf[b, pl.ds(0, n_rows)] = ((g + g * jnp.tanh(g)) * up[:, at]).astype(BF16)
                put(n + b, b).start()
        for b in range(2):
            put(ff // TILE - 2 + b, b).wait()

    weight(0, 0, sg_ref).start()

    def clear():
        @pl.loop(0, ff // TILE)
        def _(n):
            at = pl.ds(pl.multiple_of(n * TILE, TILE), TILE)
            for g in range(2):
                acc_s[g, :, at] = jnp.zeros((tokens, TILE), F32)
                for e in range(own):
                    acc[g, e, :, at] = jnp.zeros((total, TILE), F32)

    def real(j):
        return jnp.logical_and(j >= 0, j < units)

    @pl.loop(0, 7 * (units + 4))
    def _(t):
        u, i = t // 7, t % 7
        hop = 5 * i % 7
        back = (3 * hop - i) // 7

        @pl.when(real(u - back))
        def _():
            send(u - back, hop)

        @pl.when(t == 1)
        def _():
            clear()
        now = u - 3

        @pl.when(jnp.logical_and(i == 0, real(now)))
        def _():
            fetch(now)

        @pl.when(jnp.logical_and(i == 1, real(now)))
        def _():
            @pl.when(now == 0)
            def _():
                route()
            dispatch(now)
            shared(now)
        wrap = (6 - i) // 6

        @pl.when(jnp.logical_and(i != 1, real(now - wrap)))
        def _():
            product(now - wrap, i + 7 * wrap)

    for e in (own, *range(own)):
        finish(e)
    pltpu.make_async_copy(give, give_ref, give_sem.at[0]).wait()

    @pl.loop(0, units)
    def _(j):
        for way in range(2):
            for hop in range(CHIPS - 1):
                ring(j, way, hop).wait_send()
            for hop in range(CHIPS):
                pair(j, way, hop).wait_send()
    for hop in range(CHIPS):
        if hop < CHIPS - 1:
            note(hop, 0).wait_send()
        note(hop, 1).wait_send()


def down_scatter(
    h_ref, hs_ref, give_ref, wd_ref, sd_ref, y_ref,
    part, shared, psend, precv, outs, wbuf, rbuf,
    send_sem, recv_sem, psend_sem, precv_sem, w_sem,
):
    own, total, ff = h_ref.shape
    tokens, d = y_ref.shape
    units = d // STRIP
    sources = 2 * CHIPS
    pad = total // sources
    core, pos, right, left, partner = places()
    ahead = (right, left)
    meet((right, left, partner))

    mats = [sd_ref] + [wd_ref.at[e] for e in range(own)]
    count = len(mats)

    def weight(j, k):
        wide = pl.ds(pl.multiple_of(j * STRIP, STRIP), STRIP)
        return pltpu.make_async_copy(mats[k].at[:, wide], wbuf.at[k % 2], w_sem.at[k % 2])

    def bound(way, hop):
        return (pos - 1 - hop + 2 * CHIPS) % CHIPS if way == 0 else (pos + 1 + hop) % CHIPS

    def ring(j, way, hop):
        return pltpu.make_async_remote_copy(
            src_ref=rbuf.at[way, j, hop], dst_ref=rbuf.at[way, j, hop + 1],
            send_sem=send_sem.at[way, j, hop], recv_sem=recv_sem.at[way, j, hop],
            device_id=ahead[way], device_id_type=MESH)

    def arrival(j, way, hop):
        return pltpu.make_async_remote_copy(
            src_ref=rbuf.at[way, j, hop - 1], dst_ref=rbuf.at[way, j, hop],
            send_sem=send_sem.at[way, j, hop - 1], recv_sem=recv_sem.at[way, j, hop - 1],
            device_id=ahead[way], device_id_type=MESH)

    def pair(j):
        b = j % 2
        return pltpu.make_async_remote_copy(
            src_ref=psend.at[b], dst_ref=precv.at[b], send_sem=psend_sem.at[b],
            recv_sem=precv_sem.at[b], device_id=partner, device_id_type=MESH)

    def send(j, hop):
        for way in range(2):
            half = pl.ds(way * STRIP // 2, STRIP // 2)
            mine = part[j % DEPTH, bound(way, hop), :, half]
            if hop > 0:
                arrival(j, way, hop).wait_recv()
                mine += rbuf[way, j, hop].astype(F32)
            if hop < CHIPS - 1:
                rbuf[way, j, hop] = mine.astype(BF16)
                ring(j, way, hop).start()
            else:
                at = pl.ds(pl.multiple_of(j * STRIP + way * STRIP // 2, STRIP // 2), STRIP // 2)
                y_ref[:, at] = mine.astype(BF16)

    def product(j, k):
        weight(j, k).wait()
        if k + 1 < count:
            weight(j, k + 1).start()
        else:
            @pl.when(j + 1 < units)
            def _():
                weight(j + 1, 0).start()
        if k == 0:
            shared[...] = dot(hs_ref[...], wbuf[k % 2])
        else:
            e = k - 1
            r = dot(h_ref[e], wbuf[k % 2]).astype(BF16)
            for s in range(sources):
                outs[s, pl.ds(e * pad, pad), :] = r[s * pad:(s + 1) * pad]

    def combine(j):
        for place in range(CHIPS):
            s = core * CHIPS + place
            part[j % DEPTH, place] = tdot(give_ref[s], outs[s])
            o = (1 - core) * CHIPS + place
            psend[j % 2, place] = tdot(give_ref[o], outs[o]).astype(BF16)
        pair(j).start()
        part[j % DEPTH, pos] += shared[...]

    weight(0, 0).start()

    def when_real(j, act, *args):
        @pl.when(jnp.logical_and(j >= 0, j < units))
        def _():
            act(j, *args)

    def pair_sum(j):
        pair(j).wait()
        for place in range(CHIPS):
            part[j % DEPTH, place] += precv[j % 2, place].astype(F32)

    @pl.loop(0, units + DEPTH)
    def _(u):
        when_real(u - DEPTH, send, CHIPS - 1)
        when_real(u - 1, pair_sum)
        for i in range(7):
            hop = 2 * i % 7
            when_real(u - 1 - (4 * hop - i) // 7, send, hop)
            if 1 <= i <= count:
                when_real(u, product, i - 1)
            if i == 6:
                when_real(u, combine)

    @pl.loop(0, units)
    def _(j):
        for way in range(2):
            for hop in range(CHIPS - 1):
                ring(j, way, hop).wait_send()


def solution(mesh):
    def step(x, expert, slot, gate, w_gate, w_up, w_down, s_gate, s_up, s_down):
        members = mesh.shape["ep"]
        experts, (tokens, top) = w_gate.shape[0], expert.shape[2:]
        d, ff = w_gate.shape[1:]
        slots = 5 * tokens * top // (4 * experts)
        own = experts // members
        pad = -(-slots // 8) * 8
        rows, total = own * pad, members * pad
        units, strips = d // UNIT, d // STRIP
        dma, anywhere, vmem = pltpu.SemaphoreType.DMA, pl.BlockSpec(memory_space=pl.ANY), pl.BlockSpec(memory_space=pltpu.VMEM)

        def device(x, expert, slot, gate, w_gate, w_up, w_down, s_gate, s_up, s_down):
            x, expert, slot, gate = x[0, 0], expert[0, 0], slot[0, 0], gate[0, 0]
            code = jnp.where(slot < slots, expert * pad + slot, -1).astype(F32)
            info = jnp.concatenate([code.T, gate.astype(BF16).astype(F32).T])
            _, h, hs, give = pl.pallas_call(
                gather_up,
                name="gather_up",
                out_shape=(
                    jax.ShapeDtypeStruct((2, CHIPS, tokens, d), BF16),
                    jax.ShapeDtypeStruct((own, total, ff), BF16),
                    jax.ShapeDtypeStruct((tokens, ff), BF16),
                    jax.ShapeDtypeStruct((members, rows, tokens), BF16),
                ),
                in_specs=[anywhere, vmem] + [anywhere] * 4,
                out_specs=(anywhere,) * 4,
                scratch_shapes=[
                    pltpu.VMEM((2, own, total, ff), F32),
                    pltpu.VMEM((2, tokens, ff), F32),
                    pltpu.VMEM((members, tokens, UNIT), BF16),
                    pltpu.VMEM((own, total, UNIT), BF16),
                    pltpu.VMEM((2, UNIT, ff), BF16),
                    pltpu.VMEM((2, total, TILE), BF16),
                    pltpu.VMEM((2, CHIPS, 2 * top, tokens), F32),
                    pltpu.VMEM((members, rows, tokens), BF16),
                    pltpu.VMEM((members, rows, tokens), BF16),
                    dma((2, units, CHIPS)), dma((2, units, CHIPS)), dma((2, units, CHIPS)),
                    dma((2, units, CHIPS)), dma((2, 2, CHIPS)), dma((members,)), dma((2,)), dma((2,)), dma((1,)),
                ],
                compiler_params=pltpu.CompilerParams(
                    collective_id=0, has_side_effects=True, vmem_limit_bytes=67_043_328),
            )(x, info, w_gate, w_up, s_gate, s_up)
            y = pl.pallas_call(
                down_scatter,
                name="down_scatter",
                out_shape=jax.ShapeDtypeStruct((tokens, d), BF16),
                in_specs=[vmem] * 3 + [anywhere] * 2,
                out_specs=vmem,
                scratch_shapes=[
                    pltpu.VMEM((DEPTH, CHIPS, tokens, STRIP), F32),
                    pltpu.VMEM((tokens, STRIP), F32),
                    pltpu.VMEM((2, CHIPS, tokens, STRIP), BF16),
                    pltpu.VMEM((2, CHIPS, tokens, STRIP), BF16),
                    pltpu.VMEM((members, rows, STRIP), BF16),
                    pltpu.VMEM((2, ff, STRIP), BF16),
                    pltpu.VMEM((2, strips, CHIPS, tokens, STRIP // 2), BF16),
                    dma((2, strips, CHIPS)), dma((2, strips, CHIPS)), dma((2,)), dma((2,)), dma((2,)),
                ],
                compiler_params=pltpu.CompilerParams(
                    collective_id=1, has_side_effects=True, vmem_limit_bytes=67_043_328),
            )(h, hs, give, w_down, s_down)
            return y[None, None]

        tok, exp, rep = P("dp", "ep"), P("ep"), P()
        return jax.shard_map(
            device, mesh=mesh,
            in_specs=(tok, tok, tok, tok, exp, exp, exp, rep, rep, rep),
            out_specs=tok, check_vma=False,
        )(x, expert, slot, gate, w_gate, w_up, w_down, s_gate, s_up, s_down)

    return step
```

```python
import functools

import jax
import jax.numpy as jnp
from jax import lax
from jax.experimental import pallas as pl
from jax.experimental.pallas import tpu as pltpu
from jax.sharding import PartitionSpec as P

MESH = pl.DeviceIdType.MESH
F32, BF16 = jnp.float32, jnp.bfloat16
CHIPS = 8
HALF = 256
UNIT = 2 * HALF
TILE = 256
STRIP = 256
GATHER, SCATTER = 3, 5
DEPTH = SCATTER + 1


def dot(a, b):
    return jnp.dot(a, b, preferred_element_type=F32)


def tdot(a, b):
    return lax.dot_general(a, b, (((0,), (0,)), ((), ())), preferred_element_type=F32)


def chip_at(pos):
    return pos + pos // 4 * (11 - 2 * pos)


def places():
    me = lax.axis_index("ep")
    core, pos = me % 2, chip_at(me // 2)

    def device(pos, core):
        return (lax.axis_index("dp"), 2 * chip_at(pos) + core)

    right, left = device((pos + 1) % CHIPS, core), device((pos + CHIPS - 1) % CHIPS, core)
    return core, pos, right, left, device(pos, 1 - core)


def meet(devices):
    barrier = pltpu.get_barrier_semaphore()
    for d in devices:
        pl.semaphore_signal(barrier, inc=1, device_id=d, device_id_type=MESH)
    pl.semaphore_wait(barrier, len(devices))


def gather_up(
    x_ref, info_ref, wg_ref, wu_ref, sg_ref, su_ref, all_ref, h_ref, hs_ref, give_ref,
    acc, acc_s, xbuf, z, wbuf, hbuf, info, take, give,
    send_sem, recv_sem, psend_sem, precv_sem, info_sem, load_sem, w_sem, h_sem, give_sem,
):
    own, total, ff = acc.shape[1:]
    tokens, d = x_ref.shape
    top = info_ref.shape[0] // 2
    units = d // UNIT
    sources = 2 * CHIPS
    pad = total // sources
    core, pos, right, left, partner = places()
    ahead = (right, left)
    meet((right, left, partner))

    def origin(way, hop):
        return (pos - hop + CHIPS) % CHIPS if way == 0 else (pos + hop) % CHIPS

    def block(j, way, hop, color):
        at = pl.ds(pl.multiple_of(j * UNIT + way * HALF, HALF), HALF)
        return all_ref.at[color, origin(way, hop), :, at]

    def mine(j, way):
        return x_ref.at[:, pl.ds(pl.multiple_of(j * UNIT + way * HALF, HALF), HALF)]

    def ring(j, way, hop, src=None):
        here = block(j, way, hop, core)
        return pltpu.make_async_remote_copy(
            src_ref=here if src is None else src, dst_ref=here, send_sem=send_sem.at[way, j, hop],
            recv_sem=recv_sem.at[way, j, hop], device_id=ahead[way], device_id_type=MESH)

    def arrival(j, way, hop):
        there = block(j, way, hop, core)
        return pltpu.make_async_remote_copy(
            src_ref=there, dst_ref=there, send_sem=send_sem.at[way, j, hop - 1],
            recv_sem=recv_sem.at[way, j, hop - 1], device_id=ahead[way], device_id_type=MESH)

    def pair(j, way, hop, src=None):
        here = block(j, way, hop, core)
        return pltpu.make_async_remote_copy(
            src_ref=here if src is None else src, dst_ref=here, send_sem=psend_sem.at[way, j, hop],
            recv_sem=precv_sem.at[way, j, hop], device_id=partner, device_id_type=MESH)

    def pair_arrival(j, way, hop):
        there = block(j, way, hop, 1 - core)
        return pltpu.make_async_remote_copy(
            src_ref=there, dst_ref=there, send_sem=psend_sem.at[way, j, hop],
            recv_sem=precv_sem.at[way, j, hop], device_id=partner, device_id_type=MESH)

    def note(hop, to_pair, src=None):
        here = info.at[core, origin(0, hop)]
        return pltpu.make_async_remote_copy(
            src_ref=here if src is None else src, dst_ref=here, send_sem=info_sem.at[to_pair, 0, hop],
            recv_sem=info_sem.at[to_pair, 1, hop], device_id=partner if to_pair else right, device_id_type=MESH)

    def note_arrival(hop, to_pair):
        there = info.at[1 - core if to_pair else core, origin(0, hop)]
        n = hop if to_pair else hop - 1
        return pltpu.make_async_remote_copy(
            src_ref=there, dst_ref=there, send_sem=info_sem.at[to_pair, 0, n],
            recv_sem=info_sem.at[to_pair, 1, n], device_id=partner if to_pair else right, device_id_type=MESH)

    def load(j, color, place):
        wide = pl.ds(pl.multiple_of(j * UNIT, UNIT), UNIT)
        s = color * CHIPS + place
        return pltpu.make_async_copy(all_ref.at[color, place, :, wide], xbuf.at[s], load_sem.at[s])

    def load_own(j):
        wide = pl.ds(pl.multiple_of(j * UNIT, UNIT), UNIT)
        s = core * CHIPS + pos
        return pltpu.make_async_copy(x_ref.at[:, wide], xbuf.at[s], load_sem.at[s])

    last = 2 * own + 1

    def weight(j, k, mat):
        rows = pl.ds(pl.multiple_of(j * UNIT, UNIT), UNIT)
        return pltpu.make_async_copy(mat.at[rows, :], wbuf.at[k % 2], w_sem.at[k % 2])

    def send(j, hop):
        @pl.when(hop == 0)
        def _():
            @pl.when(j == 0)
            def _():
                note(0, 0, info_ref).start()
                note(0, 1, info_ref).start()
            for way in range(2):
                ring(j, way, 0, mine(j, way)).start()
                pair(j, way, 0, mine(j, way)).start()

        @pl.when(hop > 0)
        def _():
            @pl.when(j == 0)
            def _():
                note_arrival(hop, 0).wait_recv()
                note(hop, 0).start()
                note(hop, 1).start()
            for way in range(2):
                arrival(j, way, hop).wait_recv()
                ring(j, way, hop).start()
                pair(j, way, hop).start()

    def accumulate(lhs, w, total_ref):
        for n in range(0, ff, UNIT):
            at = pl.ds(n, UNIT)
            total_ref[:, at] += dot(lhs[...], w[:, at])

    def product(j, k):
        weight(j, k, wg_ref.at[0]).wait()
        e = (k - 1) // 2

        @pl.when(jnp.logical_and(k < last, k % 2 == 1))
        def _():
            weight(j, k + 1, wg_ref.at[e]).start()

        @pl.when(jnp.logical_and(k < last, k % 2 == 0))
        def _():
            weight(j, k + 1, wu_ref.at[e]).start()

        @pl.when(jnp.logical_and(k == last, j + 1 < units))
        def _():
            weight(j + 1, 0, sg_ref).start()
        e = (k - 2) // 2
        closing = jnp.logical_and(j == units - 1, k % 2 == 1)

        @pl.when(jnp.logical_not(closing))
        def _():
            accumulate(z.at[e], wbuf.at[k % 2], acc.at[k % 2, e])

        @pl.when(closing)
        def _():
            close(e)

    def put(e, n):
        at = pl.ds(n * UNIT, UNIT)
        return pltpu.make_async_copy(hbuf.at[n % 2], h_ref.at[e, :, at], h_sem.at[n % 2])

    def close(e):
        for n in range(ff // UNIT):
            at = pl.ds(n * UNIT, UNIT)
            if n < 2:
                @pl.when(e > 0)
                def _():
                    put(e - 1, ff // UNIT - 2 + n).wait()
            else:
                put(e, n - 2).wait()
            up = acc[1, e, :, at] + dot(z[e], wbuf[1, :, at])
            g = 0.5 * acc[0, e, :, at]
            hbuf[n % 2] = ((g + g * jnp.tanh(g)) * up).astype(BF16)
            put(e, n).start()

    def shared(j):
        weight(j, 0, sg_ref).wait()
        weight(j, 1, su_ref).start()
        accumulate(xbuf.at[core * CHIPS + pos], wbuf.at[0], acc_s.at[0])
        weight(j, 1, su_ref).wait()
        weight(j, 2, wg_ref.at[0]).start()
        accumulate(xbuf.at[core * CHIPS + pos], wbuf.at[1], acc_s.at[1])

    def route():
        note_arrival(CHIPS - 1, 0).wait_recv()
        note(CHIPS - 1, 1).start()
        for hop in range(CHIPS):
            note_arrival(hop, 1).wait_recv()
        info[core, pos] = info_ref[...]
        base = (lax.axis_index("ep") * own * pad).astype(F32)

        @pl.loop(0, sources)
        def _(s):
            here = info[s // CHIPS, s % CHIPS]
            row = lax.broadcasted_iota(jnp.int32, (own * pad, tokens), 0).astype(F32)
            picked = jnp.zeros((own * pad, tokens), F32)
            gates = jnp.zeros((own * pad, tokens), F32)
            for n in range(top):
                hit = row == here[n:n + 1] - base
                picked = jnp.where(hit, 1.0, picked)
                gates = jnp.where(hit, here[top + n:top + n + 1], gates)
            take[s] = picked.astype(BF16)
            give[s] = gates.astype(BF16)
        pltpu.make_async_copy(give, give_ref, give_sem.at[0]).start()

    def fetch_rest(j):
        for way in range(2):
            pair_arrival(j, way, CHIPS - 1).wait_recv()
        for hop in (1, CHIPS - 1):
            load(j, 1 - core, origin(0, hop)).start()

    def dispatch(j):
        load_own(j).wait()
        for hop in range(1, CHIPS):
            load(j, core, origin(0, hop)).wait()
        for hop in range(CHIPS):
            load(j, 1 - core, origin(0, hop)).wait()
        for s in range(sources):
            rows = dot(take[s], xbuf[s]).astype(BF16)
            for e in range(own):
                z[e, pl.ds(s * pad, pad), :] = rows[e * pad:(e + 1) * pad]

    def fetch(j):
        for way in range(2):
            arrival(j, way, CHIPS - 1).wait_recv()
            pair(j, way, CHIPS - 1).start()
        load_own(j).start()
        for hop in range(1, CHIPS):
            load(j, core, origin(0, hop)).start()
        for hop in range(CHIPS - 1):
            for way in range(2):
                pair_arrival(j, way, hop).wait_recv()
        for hop in (0, *range(2, CHIPS - 1)):
            load(j, 1 - core, origin(0, hop)).start()

    def finish_shared():
        for n in range(ff // UNIT):
            at = pl.ds(n * UNIT, UNIT)
            g = 0.5 * acc_s[0, :, at]
            hbuf[n % 2, pl.ds(0, tokens)] = ((g + g * jnp.tanh(g)) * acc_s[1, :, at]).astype(BF16)
            copy = pltpu.make_async_copy(
                hbuf.at[n % 2, pl.ds(0, tokens)], hs_ref.at[:, at], h_sem.at[n % 2])
            copy.start()
            copy.wait()

    weight(0, 0, sg_ref).start()

    def clear():
        @pl.loop(0, ff // TILE)
        def _(n):
            at = pl.ds(pl.multiple_of(n * TILE, TILE), TILE)
            for g in range(2):
                acc_s[g, :, at] = jnp.zeros((tokens, TILE), F32)
                for e in range(own):
                    acc[g, e, :, at] = jnp.zeros((total, TILE), F32)

    def real(j):
        return jnp.logical_and(j >= 0, j < units)

    @pl.loop(0, 7 * (units + GATHER + 1))
    def _(t):
        u, i = t // 7, t % 7
        hop = pow(GATHER, -1, 7) * i % 7
        back = (GATHER * hop - i) // 7

        @pl.when(real(u - back))
        def _():
            send(u - back, hop)

        @pl.when(t == 1)
        def _():
            clear()
        now = u - GATHER

        @pl.when(jnp.logical_and(i == 0, real(now)))
        def _():
            fetch(now)

        @pl.when(jnp.logical_and(i == 1, real(now)))
        def _():
            fetch_rest(now)

        @pl.when(jnp.logical_and(i == 2, real(now)))
        def _():
            @pl.when(now == 0)
            def _():
                route()
            dispatch(now)
            shared(now)
        wrap = (8 - i) // 7

        @pl.when(jnp.logical_and(i != 2, real(now - wrap)))
        def _():
            product(now - wrap, i - 1 + 7 * wrap)

    for n in (ff // UNIT - 2, ff // UNIT - 1):
        put(own - 1, n).wait()
    finish_shared()
    pltpu.make_async_copy(give, give_ref, give_sem.at[0]).wait()

    @pl.loop(0, units)
    def _(j):
        for way in range(2):
            for hop in range(CHIPS - 1):
                ring(j, way, hop).wait_send()
            for hop in range(CHIPS):
                pair(j, way, hop).wait_send()
    for hop in range(CHIPS):
        if hop < CHIPS - 1:
            note(hop, 0).wait_send()
        note(hop, 1).wait_send()


def down_scatter(
    h_ref, hs_ref, give_ref, wd_ref, sd_ref, y_ref,
    part, shared, psend, precv, outs, wbuf, rbuf,
    send_sem, recv_sem, psend_sem, precv_sem, w_sem,
):
    own, total, ff = h_ref.shape
    tokens, d = y_ref.shape
    units = d // STRIP
    sources = 2 * CHIPS
    pad = total // sources
    core, pos, right, left, partner = places()
    ahead = (right, left)
    meet((right, left, partner))

    mats = [sd_ref] + [wd_ref.at[e] for e in range(own)]
    count = len(mats)

    def weight(j, k):
        wide = pl.ds(pl.multiple_of(j * STRIP, STRIP), STRIP)
        return pltpu.make_async_copy(mats[k].at[:, wide], wbuf.at[k % 2], w_sem.at[k % 2])

    def bound(way, hop):
        return (pos - 1 - hop + 2 * CHIPS) % CHIPS if way == 0 else (pos + 1 + hop) % CHIPS

    def ring(j, way, hop):
        return pltpu.make_async_remote_copy(
            src_ref=rbuf.at[way, j, hop], dst_ref=rbuf.at[way, j, hop + 1],
            send_sem=send_sem.at[way, j, hop], recv_sem=recv_sem.at[way, j, hop],
            device_id=ahead[way], device_id_type=MESH)

    def arrival(j, way, hop):
        return pltpu.make_async_remote_copy(
            src_ref=rbuf.at[way, j, hop - 1], dst_ref=rbuf.at[way, j, hop],
            send_sem=send_sem.at[way, j, hop - 1], recv_sem=recv_sem.at[way, j, hop - 1],
            device_id=ahead[way], device_id_type=MESH)

    def pair(j):
        b = j % 2
        return pltpu.make_async_remote_copy(
            src_ref=psend.at[b], dst_ref=precv.at[b], send_sem=psend_sem.at[b],
            recv_sem=precv_sem.at[b], device_id=partner, device_id_type=MESH)

    def send(j, hop):
        for way in range(2):
            half = pl.ds(way * STRIP // 2, STRIP // 2)
            mine = part[j % DEPTH, bound(way, hop), :, half]
            if hop > 0:
                arrival(j, way, hop).wait_recv()
                mine += rbuf[way, j, hop].astype(F32)
            if hop < CHIPS - 1:
                rbuf[way, j, hop] = mine.astype(BF16)
                ring(j, way, hop).start()
            else:
                at = pl.ds(pl.multiple_of(j * STRIP + way * STRIP // 2, STRIP // 2), STRIP // 2)
                y_ref[:, at] = mine.astype(BF16)

    def product(j, k):
        weight(j, k).wait()
        if k + 1 < count:
            weight(j, k + 1).start()
        else:
            @pl.when(j + 1 < units)
            def _():
                weight(j + 1, 0).start()
        if k == 0:
            shared[...] = dot(hs_ref[...], wbuf[k % 2])
        else:
            e = k - 1
            r = dot(h_ref[e], wbuf[k % 2]).astype(BF16)
            for s in range(sources):
                outs[s, pl.ds(e * pad, pad), :] = r[s * pad:(s + 1) * pad]

    def combine(j):
        for place in range(CHIPS):
            s = core * CHIPS + place
            part[j % DEPTH, place] = tdot(give_ref[s], outs[s])
            o = (1 - core) * CHIPS + place
            psend[j % 2, place] = tdot(give_ref[o], outs[o]).astype(BF16)
        pair(j).start()
        part[j % DEPTH, pos] += shared[...]

    weight(0, 0).start()

    def when_real(j, act, *args):
        @pl.when(jnp.logical_and(j >= 0, j < units))
        def _():
            act(j, *args)

    def pair_sum(j):
        pair(j).wait()
        for place in range(CHIPS):
            part[j % DEPTH, place] += precv[j % 2, place].astype(F32)

    @pl.loop(0, units + DEPTH)
    def _(u):
        when_real(u - DEPTH, send, CHIPS - 1)
        when_real(u - 1, pair_sum)
        for i in range(7):
            hop = pow(SCATTER, -1, 7) * i % 7
            when_real(u - 1 - (SCATTER * hop - i) // 7, send, hop)
            if 1 <= i <= count:
                when_real(u, product, i - 1)
            if i == 6:
                when_real(u, combine)

    @pl.loop(0, units)
    def _(j):
        for way in range(2):
            for hop in range(CHIPS - 1):
                ring(j, way, hop).wait_send()


def solution(mesh):
    def step(x, expert, slot, gate, w_gate, w_up, w_down, s_gate, s_up, s_down):
        members = mesh.shape["ep"]
        experts, (tokens, top) = w_gate.shape[0], expert.shape[2:]
        d, ff = w_gate.shape[1:]
        slots = 5 * tokens * top // (4 * experts)
        own = experts // members
        pad = -(-slots // 8) * 8
        rows, total = own * pad, members * pad
        units, strips = d // UNIT, d // STRIP
        dma, anywhere, vmem = pltpu.SemaphoreType.DMA, pl.BlockSpec(memory_space=pl.ANY), pl.BlockSpec(memory_space=pltpu.VMEM)

        def device(x, expert, slot, gate, w_gate, w_up, w_down, s_gate, s_up, s_down):
            x, expert, slot, gate = x[0, 0], expert[0, 0], slot[0, 0], gate[0, 0]
            code = jnp.where(slot < slots, expert * pad + slot, -1).astype(F32)
            info = jnp.concatenate([code.T, gate.astype(BF16).astype(F32).T])
            _, h, hs, give = pl.pallas_call(
                gather_up,
                name="gather_up",
                out_shape=(
                    jax.ShapeDtypeStruct((2, CHIPS, tokens, d), BF16),
                    jax.ShapeDtypeStruct((own, total, ff), BF16),
                    jax.ShapeDtypeStruct((tokens, ff), BF16),
                    jax.ShapeDtypeStruct((members, rows, tokens), BF16),
                ),
                in_specs=[anywhere, vmem] + [anywhere] * 4,
                out_specs=(anywhere,) * 4,
                scratch_shapes=[
                    pltpu.VMEM((2, own, total, ff), F32),
                    pltpu.VMEM((2, tokens, ff), F32),
                    pltpu.VMEM((members, tokens, UNIT), BF16),
                    pltpu.VMEM((own, total, UNIT), BF16),
                    pltpu.VMEM((2, UNIT, ff), BF16),
                    pltpu.VMEM((2, total, UNIT), BF16),
                    pltpu.VMEM((2, CHIPS, 2 * top, tokens), F32),
                    pltpu.VMEM((members, rows, tokens), BF16),
                    pltpu.VMEM((members, rows, tokens), BF16),
                    dma((2, units, CHIPS)), dma((2, units, CHIPS)), dma((2, units, CHIPS)),
                    dma((2, units, CHIPS)), dma((2, 2, CHIPS)), dma((members,)), dma((2,)), dma((2,)), dma((1,)),
                ],
                compiler_params=pltpu.CompilerParams(
                    collective_id=0, has_side_effects=True, vmem_limit_bytes=67_043_328),
            )(x, info, w_gate, w_up, s_gate, s_up)
            y = pl.pallas_call(
                down_scatter,
                name="down_scatter",
                out_shape=jax.ShapeDtypeStruct((tokens, d), BF16),
                in_specs=[vmem] * 3 + [anywhere] * 2,
                out_specs=vmem,
                scratch_shapes=[
                    pltpu.VMEM((DEPTH, CHIPS, tokens, STRIP), F32),
                    pltpu.VMEM((tokens, STRIP), F32),
                    pltpu.VMEM((2, CHIPS, tokens, STRIP), BF16),
                    pltpu.VMEM((2, CHIPS, tokens, STRIP), BF16),
                    pltpu.VMEM((members, rows, STRIP), BF16),
                    pltpu.VMEM((2, ff, STRIP), BF16),
                    pltpu.VMEM((2, strips, CHIPS, tokens, STRIP // 2), BF16),
                    dma((2, strips, CHIPS)), dma((2, strips, CHIPS)), dma((2,)), dma((2,)), dma((2,)),
                ],
                compiler_params=pltpu.CompilerParams(
                    collective_id=1, has_side_effects=True, vmem_limit_bytes=67_043_328),
            )(h, hs, give, w_down, s_down)
            return y[None, None]

        tok, exp, rep = P("dp", "ep"), P("ep"), P()
        return jax.shard_map(
            device, mesh=mesh,
            in_specs=(tok, tok, tok, tok, exp, exp, exp, rep, rep, rep),
            out_specs=tok, check_vma=False,
        )(x, expert, slot, gate, w_gate, w_up, w_down, s_gate, s_up, s_down)

    return step
```
